256 devices in a mesh: dp: 2 (over core), expert: 32 (over z_hi, y, x), tensor: 4 (over z_lo).
Axes of the slice: x: 4, y: 4, z: 8 (z_hi: 2, z_lo: 4; z = z_hi * 4 + z_lo), core: 2. Of those that a mesh axis runs over, the one named last changes fastest.
Arguments:
- grad_out: bfloat16 [8192, 3584], P(('dp', 'expert')), may hold values from -6 to 6
- layer_in: bfloat16 [8192, 3584], P(('dp', 'expert')), may hold values from -6 to 6
- routes: int32 [8192, 8], P(('dp', 'expert')), may hold values from 0 to 255, as said below
- combine: float32 [8192, 8], P(('dp', 'expert')), may hold values from 0.2 to 1
- gate_weight: bfloat16 [32, 3584, 1024], P('expert', 'dp', 'tensor'), may hold values from -0.09375 to 0.09375
- up_weight: bfloat16 [32, 3584, 1024], P('expert', 'dp', 'tensor'), may hold values from -0.09375 to 0.09375
- down_weight: bfloat16 [32, 1024, 3584], P('expert', 'tensor', 'dp'), may hold values from -0.1875 to 0.1875
Outputs:
- grad_in: bfloat16 [8192, 3584], P(('dp', 'expert'))
- grad_gate: bfloat16 [32, 3584, 1024], P('expert', 'dp', 'tensor')
- grad_up: bfloat16 [32, 3584, 1024], P('expert', 'dp', 'tensor')
- grad_down: bfloat16 [32, 1024, 3584], P('expert', 'tensor', 'dp')
The draws below stay inside these ranges and needn't reach their ends.
Inputs may be any that keep to these rules, and one draw needn't show every extreme that they name: `routes`: each row names 8 different experts. In every block of 128 tokens (the tokens of one device) each expert below 32 is named by 1 to 8 tokens, and one such expert, the same for all blocks of a draw, is named by exactly 8 tokens of every block.
All inputs are finite; a program needn't handle non-finite values.
Results may differ from the reference program's by a relative error of at most 0.011.
Values may be sent and summed in bfloat16 or wider, within the bound.
No kernel may reach another device: no remote copies, remote signals or barrier semaphores. Data moves between devices by JAX's collectives and lax.ppermute only.
A program may use at most 128 MiB of HBM per device.

```python
import jax
import jax.numpy as jnp
from jax import lax

D = 3584
FF = 1024
ROUTED = 256
TOP = 8
TOK_DEV = 128
CAP = 8
EXPERTS = 32
TOKENS = 8192
N_DP = 2
N_EXPERT = 32
N_TENSOR = 4


def draw_routes(key, part):
    blocks = TOKENS // TOK_DEV
    subkeys = jax.random.split(jax.random.fold_in(key, 17), 5)
    labels = jnp.arange(EXPERTS, dtype=jnp.int32)
    lowest = max(CAP // 3, 1)
    counts = jax.random.randint(subkeys[0], (blocks, EXPERTS), lowest, CAP + 1).astype(jnp.int32)
    fullest = jax.random.randint(subkeys[1], (), 0, EXPERTS).astype(jnp.int32)
    counts = jnp.where(labels[None, :] == fullest, CAP, counts).astype(jnp.int32)
    residue = labels % TOP
    earlier = ((residue[:, None] == residue[None, :]) & (labels[:, None] < labels[None, :])).astype(jnp.int32)
    starts = jnp.sum(counts[:, :, None] * earlier[None, :, :], axis=1).astype(jnp.int32)
    scores = jax.random.randint(subkeys[2], (blocks, TOP, TOK_DEV), 0, 2 ** 20).astype(jnp.int32) * TOK_DEV + jnp.arange(TOK_DEV, dtype=jnp.int32)
    ranking = jnp.argsort(jnp.argsort(scores, axis=2), axis=2).astype(jnp.int32)
    rank_expert = jnp.take(ranking, residue, axis=1)
    inside = (rank_expert >= starts[:, :, None]) & (rank_expert < (starts + counts)[:, :, None])
    member = (residue[:, None] == jnp.arange(TOP, dtype=jnp.int32)[None, :]).astype(jnp.int32)
    inside_ints = jnp.transpose(inside.astype(jnp.int32), (0, 2, 1))
    found_one = jnp.sum(inside_ints[:, :, :, None] * member[None, None, :, :], axis=2)
    chosen_ids = jnp.sum((inside_ints * labels[None, None, :])[:, :, :, None] * member[None, None, :, :], axis=2)
    spare_ids = ROUTED - EXPERTS
    offset = jax.random.randint(subkeys[3], (blocks, TOK_DEV, 1), 0, spare_ids).astype(jnp.int32)
    others = EXPERTS + (offset + jnp.arange(TOP, dtype=jnp.int32)[None, None, :]) % spare_ids
    expert_ids = jnp.where(found_one > 0, chosen_ids, others).astype(jnp.int32)
    order_scores = jax.random.randint(subkeys[4], (blocks, TOK_DEV, TOP), 0, 2 ** 20).astype(jnp.int32) * TOP + jnp.arange(TOP, dtype=jnp.int32)
    shuffle = jnp.argsort(order_scores, axis=2)
    expert_ids = jnp.take_along_axis(expert_ids, shuffle, axis=2)
    return expert_ids.reshape(TOKENS, TOP).astype(jnp.int32)


def shard_levels(key, extent, shards, smallest, largest):
    level, own = 1.0, jax.random.fold_in(key, 6)
    for dim, parts in shards:
        heights = jnp.exp(jax.random.uniform(jax.random.fold_in(own, dim), (parts,), jnp.float32, smallest / len(shards), largest / len(shards)))
        level = level * jnp.repeat(heights, extent[dim] // parts).reshape([-1 if axis == dim else 1 for axis in range(len(extent))])
    return level


def centred(key, extent, spread, reach, cuts=(), kind=jnp.bfloat16):
    result = spread * jax.random.normal(key, extent, jnp.float32)
    if cuts:
        result = result * shard_levels(key, extent, cuts, -0.22, 0.18)
    return jnp.clip(result, -reach, reach).astype(kind)


def setup_inputs(seed: int = 0) -> dict:
    arg_keys = jax.random.split(jax.random.key(seed), 8)
    return {
        "grad_out": centred(arg_keys[0], (TOKENS, D), 1.0, 6.0, ((0, 64),)),
        "layer_in": centred(arg_keys[1], (TOKENS, D), 1.0, 6.0, ((0, 64),)),
        "routes": draw_routes(jax.random.fold_in(arg_keys[7], 71), 0),
        "combine": jnp.clip(0.2 + 0.8 * jax.random.uniform(arg_keys[3], (TOKENS, TOP), jnp.float32) ** shard_levels(arg_keys[3], (TOKENS, TOP), ((0, 64),), -0.2, 0.2), 0.2, 1.0),
        "gate_weight": centred(arg_keys[4], (EXPERTS, D, FF), D ** -0.5, 0.09375, ((0, 32), (1, 2), (2, 4))),
        "up_weight": centred(arg_keys[5], (EXPERTS, D, FF), D ** -0.5, 0.09375, ((0, 32), (1, 2), (2, 4))),
        "down_weight": centred(arg_keys[6], (EXPERTS, FF, D), FF ** -0.5, 0.1875, ((0, 32), (1, 4), (2, 2))),
    }


def expert_backward(in_rows, grad_rows, gate_w, up_w, down_w):
    gate = jnp.dot(in_rows, gate_w, preferred_element_type=jnp.float32)
    up = jnp.dot(in_rows, up_w, preferred_element_type=jnp.float32)
    sigma = jax.nn.sigmoid(gate)
    silu_gate = gate * sigma
    act = (silu_gate * up).astype(jnp.bfloat16)
    dhid = lax.dot_general(grad_rows, down_w, (((1,), (1,)), ((), ())), preferred_element_type=jnp.float32)
    d_up = (dhid * silu_gate).astype(jnp.bfloat16)
    d_gate = (dhid * up * sigma * (1.0 + gate * (1.0 - sigma))).astype(jnp.bfloat16)
    return act, d_gate, d_up


def reference(grad_out, layer_in, routes, combine, gate_weight, up_weight, down_weight):
    experts = gate_weight.shape[0]
    tokens, width = grad_out.shape
    blocks = tokens // TOK_DEV
    labels = jnp.arange(experts, dtype=jnp.int32)
    hits = routes[:, :, None] == labels[None, None, :]
    chosen = jnp.sum(hits, axis=1, dtype=jnp.int32)
    per_block = chosen.reshape(blocks, TOK_DEV, experts)
    before = (jnp.cumsum(per_block, axis=1) - per_block).reshape(tokens, experts).astype(jnp.int32)
    block_of = jnp.arange(tokens, dtype=jnp.int32) // TOK_DEV
    slot_of = (labels[None, :] * blocks + block_of[:, None]) * CAP + before
    dump_row = experts * blocks * CAP
    target = jnp.where(chosen > 0, slot_of, dump_row).astype(jnp.int32)
    token_ids = jnp.broadcast_to(jnp.arange(tokens, dtype=jnp.int32)[:, None] + 1, target.shape)
    owner = jnp.zeros((dump_row + 1,), jnp.int32).at[target.reshape(-1)].set(token_ids.reshape(-1))[:dump_row] - 1
    scale_of = jnp.sum(jnp.where(hits, combine[:, :, None], jnp.zeros((), jnp.float32)), axis=1)
    factor = jnp.zeros((dump_row + 1,), jnp.float32).at[target.reshape(-1)].set(scale_of.reshape(-1))[:dump_row]
    owner = owner.reshape(experts, blocks * CAP)
    factor = factor.reshape(experts, blocks * CAP)
    group_width = FF // N_TENSOR
    replica_rows = N_EXPERT * CAP

    def one_expert(items):
        owner_row, factor_row, gate_w, up_w, down_w = items
        valid = owner_row >= 0
        safe = jnp.maximum(owner_row, 0)
        in_rows = jnp.where(valid[:, None], layer_in[safe], jnp.zeros((), jnp.bfloat16))
        grad_rows = (grad_out[safe].astype(jnp.float32) * factor_row[:, None]).astype(jnp.bfloat16)
        act, d_gate, d_up = expert_backward(in_rows, grad_rows, gate_w, up_w, down_w)
        row_total = jnp.zeros(in_rows.shape, jnp.float32)
        for group in range(N_TENSOR):
            lo_col = group * group_width
            term = lax.dot_general(d_gate[:, lo_col:lo_col + group_width], gate_w[:, lo_col:lo_col + group_width], (((1,), (1,)), ((), ())), preferred_element_type=jnp.float32)
            term = term + lax.dot_general(d_up[:, lo_col:lo_col + group_width], up_w[:, lo_col:lo_col + group_width], (((1,), (1,)), ((), ())), preferred_element_type=jnp.float32)
            row_total = row_total + lax.optimization_barrier(term.astype(jnp.bfloat16)).astype(jnp.float32)
        gate_total = jnp.zeros(gate_w.shape, jnp.float32)
        up_total = jnp.zeros(up_w.shape, jnp.float32)
        down_total = jnp.zeros(down_w.shape, jnp.float32)
        for replica in range(N_DP):
            lo_row = replica * replica_rows
            rows_in = in_rows[lo_row:lo_row + replica_rows]
            part_gate = lax.dot_general(rows_in, d_gate[lo_row:lo_row + replica_rows], (((0,), (0,)), ((), ())), preferred_element_type=jnp.float32) * 0.25
            part_up = lax.dot_general(rows_in, d_up[lo_row:lo_row + replica_rows], (((0,), (0,)), ((), ())), preferred_element_type=jnp.float32) * 0.25
            part_down = lax.dot_general(act[lo_row:lo_row + replica_rows], grad_rows[lo_row:lo_row + replica_rows], (((0,), (0,)), ((), ())), preferred_element_type=jnp.float32) * 0.25
            gate_total = gate_total + lax.optimization_barrier(part_gate.astype(jnp.bfloat16)).astype(jnp.float32)
            up_total = up_total + lax.optimization_barrier(part_up.astype(jnp.bfloat16)).astype(jnp.float32)
            down_total = down_total + lax.optimization_barrier(part_down.astype(jnp.bfloat16)).astype(jnp.float32)
        return (row_total.astype(jnp.bfloat16), gate_total.astype(jnp.bfloat16), up_total.astype(jnp.bfloat16), down_total.astype(jnp.bfloat16))

    rows_all, grad_gate, grad_up, grad_down = lax.map(one_expert, (owner, factor, gate_weight, up_weight, down_weight))
    pair_pos = jnp.sum(jnp.where(hits, slot_of[:, None, :], 0), axis=2) + dump_row * (1 - jnp.sum(hits, axis=2, dtype=jnp.int32))
    pair_pos = pair_pos.astype(jnp.int32)
    row_table = jnp.concatenate([rows_all.reshape(dump_row, width), jnp.zeros((1, width), jnp.bfloat16)], axis=0)
    total = jnp.zeros((tokens, width), jnp.float32)
    for choice_index in range(TOP):
        total = total + row_table[pair_pos[:, choice_index]].astype(jnp.float32)
    return (total.astype(jnp.bfloat16), grad_gate, grad_up, grad_down)
```

```python
import jax
import jax.numpy as jnp
from jax import lax
from jax.sharding import PartitionSpec as P

CAP = 8
BF = jnp.bfloat16
F32 = jnp.float32


def dot(a, b, ca, cb):
    return lax.dot_general(a, b, (((ca,), (cb,)), ((), ())), preferred_element_type=F32)


def slot_tables(routes, combine, experts):
    tokens = routes.shape[0]
    hits = routes.T[None, :, :] == jnp.arange(experts, dtype=jnp.int32)[:, None, None]
    chosen = jnp.sum(hits.astype(F32), axis=1)
    scale = jnp.sum(jnp.where(hits, combine.T[None, :, :], 0.0), axis=1)
    ids = jnp.arange(tokens, dtype=jnp.int32)
    earlier = (ids[:, None] < ids[None, :]).astype(BF)
    before = jnp.dot(chosen.astype(BF), earlier, preferred_element_type=F32)
    slots = jnp.arange(CAP, dtype=F32)
    taken = (before[:, None, :] == slots[None, :, None]) & (chosen[:, None, :] > 0)
    factor = jnp.sum(jnp.where(taken, scale[:, None, :], 0.0), axis=2)
    return taken.astype(BF).reshape(experts * CAP, tokens), factor


def swap(x):
    return lax.ppermute(x, "dp", [(0, 1), (1, 0)])


def both_halves(mine, axis):
    other = swap(mine)
    first = lax.axis_index("dp") == 0
    return jnp.concatenate(
        [jnp.where(first, mine, other), jnp.where(first, other, mine)], axis=axis
    )


def body(grad_out, layer_in, routes, combine, gate_weight, up_weight, down_weight):
    experts = lax.axis_size("expert")
    n_tensor = lax.axis_size("tensor")
    tokens, width = grad_out.shape
    rows = experts * CAP
    half = width // 2
    part = width // n_tensor
    my_dp = lax.axis_index("dp")
    my_t = lax.axis_index("tensor")

    gate_full = both_halves(gate_weight[0], 0)
    up_full = both_halves(up_weight[0], 0)
    down_full = both_halves(down_weight[0], 1)

    picker, factor = slot_tables(routes, combine, experts)
    in_rows = jnp.dot(picker, layer_in, preferred_element_type=F32).astype(BF)
    grad_rows = jnp.dot(picker, grad_out, preferred_element_type=F32)
    grad_rows = (grad_rows * factor.reshape(rows, 1)).astype(BF)
    sent = jnp.concatenate(
        [in_rows.reshape(experts, CAP, width), grad_rows.reshape(experts, CAP, width)], axis=1
    )
    got = lax.all_to_all(sent, "expert", split_axis=0, concat_axis=0, tiled=True)
    in_rows = got[:, :CAP].reshape(rows, width)
    grad_rows = got[:, CAP:].reshape(rows, width)

    gate = dot(in_rows, gate_full, 1, 0)
    up = dot(in_rows, up_full, 1, 0)
    dhid = dot(grad_rows, down_full, 1, 1)
    sigma = jax.nn.sigmoid(gate)
    silu_gate = gate * sigma
    act = (silu_gate * up).astype(BF)
    d_up = (dhid * silu_gate).astype(BF)
    d_gate = (dhid * up * sigma * (1.0 + gate * (1.0 - sigma))).astype(BF)

    def row_part(index):
        g = lax.dynamic_slice_in_dim(gate_full, index * part, part, axis=0)
        u = lax.dynamic_slice_in_dim(up_full, index * part, part, axis=0)
        return (dot(d_gate, g, 1, 1) + dot(d_up, u, 1, 1)).astype(BF)

    received = []
    for step in (2, 1, 3):
        piece = row_part((my_t + step) % n_tensor)
        received.append(
            lax.ppermute(piece, "tensor", [(i, (i + step) % n_tensor) for i in range(n_tensor)])
        )
    row_sum = row_part(my_t).astype(F32)
    for piece in received:
        row_sum = row_sum + piece.astype(F32)
    returned = lax.all_to_all(
        row_sum.astype(BF).reshape(experts, CAP, part),
        "expert",
        split_axis=0,
        concat_axis=0,
        tiled=True,
    )
    total = dot(picker, returned.reshape(rows, part), 0, 0).astype(BF)
    total = lax.all_gather(total, "tensor", axis=0, tiled=False)
    total = jnp.transpose(total, (1, 0, 2)).reshape(tokens, width)

    mine_at = my_dp * half
    other_at = (1 - my_dp) * half

    def columns(x, at):
        return lax.dynamic_slice_in_dim(x, at, half, axis=1)

    in_other, in_mine = columns(in_rows, other_at), columns(in_rows, mine_at)
    gr_other, gr_mine = columns(grad_rows, other_at), columns(grad_rows, mine_at)

    def term(a, b):
        return (dot(a, b, 0, 0) * 0.25).astype(BF)

    def finish(a_other, a_mine, b_other, b_mine):
        got_term = swap(term(a_other, b_other))
        return (term(a_mine, b_mine).astype(F32) + got_term.astype(F32)).astype(BF)

    grad_gate = finish(in_other, in_mine, d_gate, d_gate)
    grad_up = finish(in_other, in_mine, d_up, d_up)
    grad_down = finish(act, act, gr_other, gr_mine)
    return total, grad_gate[None], grad_up[None], grad_down[None]


def solution(mesh):
    return jax.shard_map(
        body,
        mesh=mesh,
        in_specs=(
            P(("dp", "expert"), None),
            P(("dp", "expert"), None),
            P(("dp", "expert"), None),
            P(("dp", "expert"), None),
            P("expert", "dp", "tensor"),
            P("expert", "dp", "tensor"),
            P("expert", "tensor", "dp"),
        ),
        out_specs=(
            P(("dp", "expert"), None),
            P("expert", "dp", "tensor"),
            P("expert", "dp", "tensor"),
            P("expert", "tensor", "dp"),
        ),
        check_vma=False,
    )
```

```python
import jax
import jax.numpy as jnp
from jax import lax
from jax.sharding import Mesh
from jax.sharding import PartitionSpec as P


CAP = 8
BF = jnp.bfloat16
F32 = jnp.float32


def dot(a, b, ca, cb):
    return lax.dot_general(a, b, (((ca,), (cb,)), ((), ())), preferred_element_type=F32)


def slot_tables(routes_t, combine_t, labels):
    tokens = routes_t.shape[1]
    experts = labels.shape[0]
    hits = routes_t[None, :, :] == labels[:, None, None]
    chosen = jnp.sum(hits.astype(F32), axis=1)
    scale = jnp.sum(jnp.where(hits, combine_t[None, :, :], 0.0), axis=1)
    ids = jnp.arange(tokens, dtype=jnp.int32)
    earlier = (ids[:, None] < ids[None, :]).astype(BF)
    before = jnp.dot(chosen.astype(BF), earlier, preferred_element_type=F32)
    slots = jnp.arange(CAP, dtype=F32)
    taken = (before[:, None, :] == slots[None, :, None]) & (chosen[:, None, :] > 0)
    factor = jnp.sum(jnp.where(taken, scale[:, None, :], 0.0), axis=2)
    return taken.astype(BF).reshape(experts * CAP, tokens), factor.reshape(experts * CAP, 1)


def pick(picker, x):
    return jnp.dot(picker, x, preferred_element_type=F32).astype(BF)


def pick_scaled(picker, x, factor):
    return (jnp.dot(picker, x, preferred_element_type=F32) * factor).astype(BF)


def swap(x, axis):
    return lax.ppermute(x, axis, [(0, 1), (1, 0)])


def both_halves(mine, axis):
    other = swap(mine, "dp")
    first = lax.axis_index("dp") == 0
    return jnp.concatenate(
        [jnp.where(first, mine, other), jnp.where(first, other, mine)], axis=axis
    )


def cross_quarter(x, part):
    t = lax.axis_index("tensor")
    n = lax.axis_size("tensor")
    last = n - 1

    def piece(low, high):
        at = jnp.where(t == last, low, high) * part
        return lax.dynamic_slice_in_dim(x, at, part, axis=1)

    out = None
    for k in range(n // 2):
        perm = []
        for z in range(2):
            perm.append((z * n + last, (1 - z) * n + k))
            perm.append((z * n, (1 - z) * n + last - k))
        got = lax.ppermute(piece(k, last - k), ("zh", "tensor"), perm)
        out = got if out is None else out + got
    return out


def gather_quarters(q):
    n = lax.axis_size("tensor")
    tokens, part = q.shape
    full = lax.all_gather(q, "tensor", axis=0, tiled=False)
    return jnp.transpose(full, (1, 0, 2)).reshape(tokens, n * part)


def gradients_of_units(in_rows, grad_rows, gate_full, up_full, down_full):
    gate = dot(in_rows, gate_full, 1, 0)
    up = dot(in_rows, up_full, 1, 0)
    dhid = dot(grad_rows, down_full, 1, 1)
    sigma = jax.nn.sigmoid(gate)
    silu_gate = gate * sigma
    act = (silu_gate * up).astype(BF)
    d_up = (dhid * silu_gate).astype(BF)
    d_gate = (dhid * up * sigma * (1.0 + gate * (1.0 - sigma))).astype(BF)
    return act, d_gate, d_up


def reduced_rows(d_gate, d_up, gate_full, up_full, part):
    n = lax.axis_size("tensor")
    t = lax.axis_index("tensor")

    def row_part(index):
        g = lax.dynamic_slice_in_dim(gate_full, index * part, part, axis=0)
        u = lax.dynamic_slice_in_dim(up_full, index * part, part, axis=0)
        return dot(d_gate, g, 1, 1) + dot(d_up, u, 1, 1)

    received = []
    for step in (2, 1, 3):
        piece = row_part((t + step) % n).astype(BF)
        received.append(lax.ppermute(piece, "tensor", [(i, (i + step) % n) for i in range(n)]))
    total = row_part(t)
    for piece in received:
        total = total + piece.astype(F32)
    return total.astype(BF)


def exchange(x):
    return lax.all_to_all(x, "col", split_axis=0, concat_axis=0, tiled=True)


def inner(grad_out, layer_in, routes, combine, gate_weight, up_weight, down_weight):
    cols = lax.axis_size("col")
    n_tensor = lax.axis_size("tensor")
    _, width = grad_out.shape
    rows = cols * CAP
    half = width // 2
    part = width // n_tensor
    my_dp = lax.axis_index("dp")
    my_zh = lax.axis_index("zh")

    routes_t, combine_t = routes.T, combine.T
    far_routes, far_combine = swap(routes_t, "zh"), swap(combine_t, "zh")
    far_in_q = cross_quarter(layer_in, part)
    far_grad_q = cross_quarter(grad_out, part)

    gate_full = both_halves(gate_weight[0], 0)
    up_full = both_halves(up_weight[0], 0)
    down_full = both_halves(down_weight[0], 1)

    labels = my_zh * cols + jnp.arange(cols, dtype=jnp.int32)
    picker, factor = slot_tables(routes_t, combine_t, labels)
    sent = jnp.concatenate(
        [
            pick(picker, layer_in).reshape(cols, CAP, width),
            pick_scaled(picker, grad_out, factor).reshape(cols, CAP, width),
        ],
        axis=1,
    )
    got = exchange(sent)
    in_rows = got[:, :CAP].reshape(rows, width)
    grad_rows = got[:, CAP:].reshape(rows, width)

    far_picker, far_factor = slot_tables(far_routes, far_combine, labels)
    far_in = pick(far_picker, gather_quarters(far_in_q))
    far_grad = pick_scaled(far_picker, gather_quarters(far_grad_q), far_factor)
    far_sent = [x.reshape(cols, CAP, width) for x in (far_in, far_grad)]
    far_got = exchange(jnp.concatenate(far_sent, axis=1))
    far_in = far_got[:, :CAP].reshape(rows, width)
    far_grad = far_got[:, CAP:].reshape(rows, width)

    act, d_gate, d_up = gradients_of_units(in_rows, grad_rows, gate_full, up_full, down_full)
    near_rows = reduced_rows(d_gate, d_up, gate_full, up_full, part)
    near_back = exchange(near_rows.reshape(cols, CAP, part)).reshape(rows, part)
    near_sum = dot(picker, near_back, 0, 0)

    far_act, far_d_gate, far_d_up = gradients_of_units(
        far_in, far_grad, gate_full, up_full, down_full
    )
    far_rows = reduced_rows(far_d_gate, far_d_up, gate_full, up_full, part)
    far_back = exchange(far_rows.reshape(cols, CAP, part)).reshape(rows, part)
    far_sum = dot(far_picker, far_back, 0, 0).astype(BF)
    total = (near_sum + swap(far_sum, "zh").astype(F32)).astype(BF)

    mine_at = my_dp * half
    other_at = (1 - my_dp) * half

    def columns(x, at):
        return lax.dynamic_slice_in_dim(x, at, half, axis=1)

    def finish(a, b, cut):
        a = jnp.concatenate(a, axis=0)
        b = jnp.concatenate(b, axis=0)

        def term(at):
            left, right = (columns(a, at), b) if cut == 0 else (a, columns(b, at))
            return (dot(left, right, 0, 0) * 0.25).astype(BF)

        got_term = swap(term(other_at), "dp")
        return (term(mine_at).astype(F32) + got_term.astype(F32)).astype(BF)

    grad_gate = finish((in_rows, far_in), (d_gate, far_d_gate), 0)
    grad_up = finish((in_rows, far_in), (d_up, far_d_up), 0)
    grad_down = finish((act, far_act), (grad_rows, far_grad), 1)
    total, grad_gate, grad_up, grad_down = lax.optimization_barrier(
        (total, grad_gate, grad_up, grad_down)
    )
    total = gather_quarters(total)
    return total, grad_gate[None], grad_up[None], grad_down[None]


def solution(mesh):
    n_dp, n_expert, n_tensor = (mesh.shape[a] for a in ("dp", "expert", "tensor"))
    split = Mesh(
        mesh.devices.reshape(n_dp, 2, n_expert // 2, n_tensor), ("dp", "zh", "col", "tensor")
    )
    blocks = P(("dp", "zh", "col"), None)
    by_rows = P(("zh", "col"), "dp", "tensor")
    by_columns = P(("zh", "col"), "tensor", "dp")
    return jax.shard_map(
        inner,
        mesh=split,
        in_specs=(blocks, blocks, blocks, blocks, by_rows, by_rows, by_columns),
        out_specs=(blocks, by_rows, by_rows, by_columns),
        check_vma=False,
    )
```

```python
import jax
import jax.numpy as jnp
from jax import lax
from jax.sharding import Mesh
from jax.sharding import PartitionSpec as P


CAP = 8
BF = jnp.bfloat16
F32 = jnp.float32


def dot(a, b, ca, cb):
    return lax.dot_general(a, b, (((ca,), (cb,)), ((), ())), preferred_element_type=F32)


def slot_tables(routes_t, combine_t, labels):
    tokens = routes_t.shape[1]
    experts = labels.shape[0]
    hits = routes_t[None, :, :] == labels[:, None, None]
    chosen = jnp.sum(hits.astype(F32), axis=1)
    scale = jnp.sum(jnp.where(hits, combine_t[None, :, :], 0.0), axis=1)
    ids = jnp.arange(tokens, dtype=jnp.int32)
    earlier = (ids[:, None] < ids[None, :]).astype(BF)
    before = jnp.dot(chosen.astype(BF), earlier, preferred_element_type=F32)
    slots = jnp.arange(CAP, dtype=F32)
    taken = (before[:, None, :] == slots[None, :, None]) & (chosen[:, None, :] > 0)
    factor = jnp.sum(jnp.where(taken, scale[:, None, :], 0.0), axis=2)
    return taken.astype(BF).reshape(experts * CAP, tokens), factor.reshape(experts * CAP, 1)


def pick(picker, x):
    return jnp.dot(picker, x, preferred_element_type=F32).astype(BF)


def pick_scaled(picker, x, factor):
    return (jnp.dot(picker, x, preferred_element_type=F32) * factor).astype(BF)


def swap(x, axis):
    return lax.ppermute(x, axis, [(0, 1), (1, 0)])


def both_halves(mine, axis):
    other = swap(mine, "dp")
    first = lax.axis_index("dp") == 0
    return lax.optimization_barrier(
        jnp.concatenate(
            [jnp.where(first, mine, other), jnp.where(first, other, mine)], axis=axis
        )
    )


def tokens_of_far_half(layer_in, grad_out):
    t = lax.axis_index("tensor")
    n = lax.axis_size("tensor")
    tokens, width = layer_in.shape
    share = tokens // n
    mine = [lax.dynamic_slice_in_dim(x, t * share, share, axis=0) for x in (layer_in, grad_out)]
    both = lax.all_gather(jnp.stack(mine), ("zh", "tensor"), axis=0, tiled=False)
    far = lax.dynamic_slice_in_dim(both, (1 - lax.axis_index("zh")) * n, n, axis=0)
    return [far[:, k].reshape(tokens, width) for k in range(2)]


def gather_quarters(q):
    n = lax.axis_size("tensor")
    tokens, part = q.shape
    full = lax.all_gather(q, "tensor", axis=0, tiled=False)
    return jnp.transpose(full, (1, 0, 2)).reshape(tokens, n * part)


def gradients_of_units(in_rows, grad_rows, gate_full, up_full, down_full):
    gate = dot(in_rows, gate_full, 1, 0)
    up = dot(in_rows, up_full, 1, 0)
    dhid = dot(grad_rows, down_full, 1, 1)
    sigma = jax.nn.sigmoid(gate)
    silu_gate = gate * sigma
    act = (silu_gate * up).astype(BF)
    d_up = (dhid * silu_gate).astype(BF)
    d_gate = (dhid * up * sigma * (1.0 + gate * (1.0 - sigma))).astype(BF)
    return act, d_gate, d_up


def reduced_rows(d_gate, d_up, gate_full, up_full, part):
    n = lax.axis_size("tensor")
    t = lax.axis_index("tensor")

    def row_part(index):
        g = lax.dynamic_slice_in_dim(gate_full, index * part, part, axis=0)
        u = lax.dynamic_slice_in_dim(up_full, index * part, part, axis=0)
        return dot(d_gate, g, 1, 1) + dot(d_up, u, 1, 1)

    received = []
    for step in (2, 1, 3):
        piece = row_part((t + step) % n).astype(BF)
        received.append(lax.ppermute(piece, "tensor", [(i, (i + step) % n) for i in range(n)]))
    total = row_part(t)
    for piece in received:
        total = total + piece.astype(F32)
    return total.astype(BF)


def exchange(x):
    return lax.all_to_all(x, "col", split_axis=0, concat_axis=0, tiled=True)


def inner(grad_out, layer_in, routes, combine, gate_weight, up_weight, down_weight):
    cols = lax.axis_size("col")
    n_tensor = lax.axis_size("tensor")
    _, width = grad_out.shape
    rows = cols * CAP
    half = width // 2
    part = width // n_tensor
    my_dp = lax.axis_index("dp")
    my_zh = lax.axis_index("zh")

    routes_t, combine_t = routes.T, combine.T
    far_routes, far_combine = swap(routes_t, "zh"), swap(combine_t, "zh")
    far_layer_in, far_grad_out = tokens_of_far_half(layer_in, grad_out)
    gate_full = both_halves(gate_weight[0], 0)
    up_full = both_halves(up_weight[0], 0)
    down_full = both_halves(down_weight[0], 1)

    labels = my_zh * cols + jnp.arange(cols, dtype=jnp.int32)
    picker, factor = slot_tables(routes_t, combine_t, labels)
    sent = jnp.concatenate(
        [
            pick(picker, layer_in).reshape(cols, CAP, width),
            pick_scaled(picker, grad_out, factor).reshape(cols, CAP, width),
        ],
        axis=1,
    )
    got = exchange(sent)
    in_rows = got[:, :CAP].reshape(rows, width)
    grad_rows = got[:, CAP:].reshape(rows, width)

    far_routes, far_combine, _ = lax.optimization_barrier((far_routes, far_combine, sent))
    far_picker, far_factor = slot_tables(far_routes, far_combine, labels)
    far_in = pick(far_picker, far_layer_in)
    far_grad = pick_scaled(far_picker, far_grad_out, far_factor)
    far_sent = [x.reshape(cols, CAP, width) for x in (far_in, far_grad)]
    far_got = exchange(jnp.concatenate(far_sent, axis=1))
    far_in = far_got[:, :CAP].reshape(rows, width)
    far_grad = far_got[:, CAP:].reshape(rows, width)

    act, d_gate, d_up = gradients_of_units(in_rows, grad_rows, gate_full, up_full, down_full)
    near_rows = reduced_rows(d_gate, d_up, gate_full, up_full, part)
    near_back = exchange(near_rows.reshape(cols, CAP, part)).reshape(rows, part)
    near_sum = dot(picker, near_back, 0, 0)

    far_act, far_d_gate, far_d_up = gradients_of_units(
        far_in, far_grad, gate_full, up_full, down_full
    )
    far_rows = reduced_rows(far_d_gate, far_d_up, gate_full, up_full, part)
    far_back = exchange(far_rows.reshape(cols, CAP, part)).reshape(rows, part)
    far_sum = dot(far_picker, far_back, 0, 0).astype(BF)
    total = (near_sum + swap(far_sum, "zh").astype(F32)).astype(BF)

    mine_at = my_dp * half
    other_at = (1 - my_dp) * half

    def columns(x, at):
        return lax.dynamic_slice_in_dim(x, at, half, axis=1)

    def finish(a, b, cut):
        a = jnp.concatenate(a, axis=0)
        b = jnp.concatenate(b, axis=0)

        def term(at):
            left, right = (columns(a, at), b) if cut == 0 else (a, columns(b, at))
            return (dot(left, right, 0, 0) * 0.25).astype(BF)

        got_term = swap(term(other_at), "dp")
        return (term(mine_at).astype(F32) + got_term.astype(F32)).astype(BF)

    grad_gate = finish((in_rows, far_in), (d_gate, far_d_gate), 0)
    grad_up = finish((in_rows, far_in), (d_up, far_d_up), 0)
    grad_down = finish((act, far_act), (grad_rows, far_grad), 1)
    total, grad_gate, grad_up, grad_down = lax.optimization_barrier(
        (total, grad_gate, grad_up, grad_down)
    )
    total = gather_quarters(total)
    return total, grad_gate[None], grad_up[None], grad_down[None]


def solution(mesh):
    n_dp, n_expert, n_tensor = (mesh.shape[a] for a in ("dp", "expert", "tensor"))
    split = Mesh(
        mesh.devices.reshape(n_dp, 2, n_expert // 2, n_tensor), ("dp", "zh", "col", "tensor")
    )
    blocks = P(("dp", "zh", "col"), None)
    by_rows = P(("zh", "col"), "dp", "tensor")
    by_columns = P(("zh", "col"), "tensor", "dp")
    return jax.shard_map(
        inner,
        mesh=split,
        in_specs=(blocks, blocks, blocks, blocks, by_rows, by_rows, by_columns),
        out_specs=(blocks, by_rows, by_rows, by_columns),
        check_vma=False,
    )
```

```python
import jax
import jax.numpy as jnp
from jax import lax
from jax.sharding import Mesh
from jax.sharding import PartitionSpec as P


CAP = 8
BF = jnp.bfloat16
F32 = jnp.float32


def dot(a, b, ca, cb):
    return lax.dot_general(a, b, (((ca,), (cb,)), ((), ())), preferred_element_type=F32)


def cut(x, index, size, axis):
    return lax.dynamic_slice_in_dim(x, index * size, size, axis=axis)


def slot_tables(routes_t, combine_t, labels):
    tokens = routes_t.shape[1]
    experts = labels.shape[0]
    hits = routes_t[None, :, :] == labels[:, None, None]
    chosen = jnp.sum(hits.astype(F32), axis=1)
    scale = jnp.sum(jnp.where(hits, combine_t[None, :, :], 0.0), axis=1)
    ids = jnp.arange(tokens, dtype=jnp.int32)
    earlier = (ids[:, None] < ids[None, :]).astype(BF)
    before = jnp.dot(chosen.astype(BF), earlier, preferred_element_type=F32)
    slots = jnp.arange(CAP, dtype=F32)
    taken = (before[:, None, :] == slots[None, :, None]) & (chosen[:, None, :] > 0)
    factor = jnp.sum(jnp.where(taken, scale[:, None, :], 0.0), axis=2)
    return taken.astype(BF).reshape(experts * CAP, tokens), factor.reshape(experts * CAP, 1)


def picked(picker, factor, layer_in, grad_out, cols):
    width = layer_in.shape[1]
    in_rows = jnp.dot(picker, layer_in, preferred_element_type=F32).astype(BF)
    grad_rows = (jnp.dot(picker, grad_out, preferred_element_type=F32) * factor).astype(BF)
    return jnp.concatenate(
        [in_rows.reshape(cols, CAP, width), grad_rows.reshape(cols, CAP, width)], axis=1
    )


def swap(x, axis):
    return lax.ppermute(x, axis, [(0, 1), (1, 0)])


def both_halves(mine, axis):
    other = swap(mine, "dp")
    first = lax.axis_index("dp") == 0
    return lax.optimization_barrier(
        jnp.concatenate(
            [jnp.where(first, mine, other), jnp.where(first, other, mine)], axis=axis
        )
    )


def exchange(x, axes):
    return lax.all_to_all(x, axes, split_axis=0, concat_axis=0, tiled=True)


def rotated(x, step):
    n = lax.axis_size("tensor")
    return lax.ppermute(x, "tensor", [(i, (i + step) % n) for i in range(n)])


def unit_gradients(gate, up, dhid):
    sigma = jax.nn.sigmoid(gate)
    silu_gate = gate * sigma
    act = (silu_gate * up).astype(BF)
    d_up = (dhid * silu_gate).astype(BF)
    d_gate = (dhid * up * sigma * (1.0 + gate * (1.0 - sigma))).astype(BF)
    return act, d_gate, d_up


def reduced_rows(d_gate, d_up, gate_full, up_full, part):
    n = lax.axis_size("tensor")
    t = lax.axis_index("tensor")

    def row_part(index):
        return dot(d_gate, cut(gate_full, index, part, 0), 1, 1) + dot(
            d_up, cut(up_full, index, part, 0), 1, 1
        )

    received = [rotated(row_part((t + s) % n).astype(BF), s) for s in (2, 1, 3)]
    total = row_part(t)
    for piece in received:
        total = total + piece.astype(F32)
    return total.astype(BF)


def inner(grad_out, layer_in, routes, combine, gate_weight, up_weight, down_weight):
    cols = lax.axis_size("col")
    n = lax.axis_size("tensor")
    tokens, width = grad_out.shape
    rows = cols * CAP
    half = width // 2
    part = width // n
    per_half = half // part
    my_dp = lax.axis_index("dp")
    my_zh = lax.axis_index("zh")
    t = lax.axis_index("tensor")

    ids = jnp.arange(cols, dtype=jnp.int32)
    labels = jnp.concatenate([my_zh * cols + ids, (1 - my_zh) * cols + ids])
    picker, factor = slot_tables(routes.T, combine.T, labels)
    near_picker, far_picker = picker[:rows], picker[rows:]

    far_sent = picked(
        far_picker, factor[rows:], cut(layer_in, t, part, 1), cut(grad_out, t, part, 1), cols
    )
    far_got = exchange(far_sent, "col")
    far_in = swap(far_got[:, :CAP].reshape(rows, part), "zh")
    far_grad = swap(far_got[:, CAP:].reshape(rows, part), "zh")

    near_got = exchange(picked(near_picker, factor[:rows], layer_in, grad_out, cols), "col")
    near_in = near_got[:, :CAP].reshape(rows, width)
    near_grad = near_got[:, CAP:].reshape(rows, width)

    gate_full = both_halves(gate_weight[0], 0)
    up_full = both_halves(up_weight[0], 0)
    down_full = both_halves(down_weight[0], 1)

    far_ins = [far_in] + [rotated(far_in, s) for s in range(1, n)]
    far_grads = [far_grad] + [rotated(far_grad, s) for s in range(1, n)]

    act, d_gate, d_up = unit_gradients(
        dot(near_in, gate_full, 1, 0),
        dot(near_in, up_full, 1, 0),
        dot(near_grad, down_full, 1, 1),
    )
    near_rows = reduced_rows(d_gate, d_up, gate_full, up_full, part)

    gate = up = dhid = 0.0
    for s in range(n):
        q = (t - s) % n
        gate = gate + dot(far_ins[s], cut(gate_full, q, part, 0), 1, 0)
        up = up + dot(far_ins[s], cut(up_full, q, part, 0), 1, 0)
        dhid = dhid + dot(far_grads[s], cut(down_full, q, part, 1), 1, 1)
    far_act, far_d_gate, far_d_up = unit_gradients(gate, up, dhid)
    far_rows = reduced_rows(far_d_gate, far_d_up, gate_full, up_full, part)

    first = my_zh == 0
    back = jnp.stack(
        [jnp.where(first, near_rows, far_rows), jnp.where(first, far_rows, near_rows)]
    )
    back = exchange(back.reshape(2 * cols, CAP, part), ("zh", "col"))
    back = back.reshape(2, rows, part)
    total = dot(near_picker, cut(back, my_zh, 1, 0)[0], 0, 0) + dot(
        far_picker, cut(back, 1 - my_zh, 1, 0)[0], 0, 0
    )
    total = total.astype(BF)

    far_in_all, far_grad_all = jnp.stack(far_ins), jnp.stack(far_grads)

    def quarter(stacked, q):
        return cut(stacked, (t - q) % n, 1, 0)[0]

    def in_term(h, near_d, far_d):
        near = dot(cut(near_in, h, half, 1), near_d, 0, 0)
        far = [dot(quarter(far_in_all, per_half * h + k), far_d, 0, 0) for k in range(per_half)]
        return ((near + jnp.concatenate(far, axis=0)) * 0.25).astype(BF)

    def down_term(h, near_a, far_a):
        near = dot(near_a, cut(near_grad, h, half, 1), 0, 0)
        far = [dot(far_a, quarter(far_grad_all, per_half * h + k), 0, 0) for k in range(per_half)]
        return ((near + jnp.concatenate(far, axis=1)) * 0.25).astype(BF)

    def finish(term, near_side, far_side):
        got_term = swap(term(1 - my_dp, near_side, far_side), "dp")
        return (term(my_dp, near_side, far_side).astype(F32) + got_term.astype(F32)).astype(BF)

    grad_gate = finish(in_term, d_gate, far_d_gate)
    grad_up = finish(in_term, d_up, far_d_up)
    grad_down = finish(down_term, act, far_act)
    total, grad_gate, grad_up, grad_down = lax.optimization_barrier(
        (total, grad_gate, grad_up, grad_down)
    )
    total = lax.all_gather(total, "tensor", axis=0, tiled=False)
    total = jnp.transpose(total, (1, 0, 2)).reshape(tokens, width)
    return total, grad_gate[None], grad_up[None], grad_down[None]


def solution(mesh):
    n_dp, n_expert, n_tensor = (mesh.shape[a] for a in ("dp", "expert", "tensor"))
    split = Mesh(
        mesh.devices.reshape(n_dp, 2, n_expert // 2, n_tensor), ("dp", "zh", "col", "tensor")
    )
    blocks = P(("dp", "zh", "col"), None)
    by_rows = P(("zh", "col"), "dp", "tensor")
    by_columns = P(("zh", "col"), "tensor", "dp")
    return jax.shard_map(
        inner,
        mesh=split,
        in_specs=(blocks, blocks, blocks, blocks, by_rows, by_rows, by_columns),
        out_specs=(blocks, by_rows, by_rows, by_columns),
        check_vma=False,
    )
```

```python
import jax
import jax.numpy as jnp
from jax import lax
from jax.sharding import Mesh
from jax.sharding import PartitionSpec as P


CAP = 8
BF = jnp.bfloat16
F32 = jnp.float32


def dot(a, b, ca, cb):
    return lax.dot_general(a, b, (((ca,), (cb,)), ((), ())), preferred_element_type=F32)


def cut(x, index, size, axis):
    return lax.dynamic_slice_in_dim(x, index * size, size, axis=axis)


def slot_tables(routes_t, combine_t, labels):
    tokens = routes_t.shape[1]
    experts = labels.shape[0]
    hits = routes_t[None, :, :] == labels[:, None, None]
    chosen = jnp.sum(hits.astype(F32), axis=1)
    ids = jnp.arange(tokens, dtype=jnp.int32)
    earlier = (ids[:, None] < ids[None, :]).astype(BF)
    before = jnp.dot(chosen.astype(BF), earlier, preferred_element_type=F32)
    slots = jnp.arange(CAP, dtype=F32)
    taken = (before[:, None, :] == slots[None, :, None]) & (chosen[:, None, :] > 0)
    picker = taken.astype(BF).reshape(experts * CAP, tokens)
    if combine_t is None:
        return picker, None
    scale = jnp.sum(jnp.where(hits, combine_t[None, :, :], 0.0), axis=1)
    factor = jnp.sum(jnp.where(taken, scale[:, None, :], 0.0), axis=2)
    return picker, factor.reshape(experts * CAP, 1)


def pick(picker, x):
    return jnp.dot(picker, x, preferred_element_type=F32).astype(BF)


def pick_scaled(picker, x, factor):
    return (jnp.dot(picker, x, preferred_element_type=F32) * factor).astype(BF)


def swap(x, axis):
    return lax.ppermute(x, axis, [(0, 1), (1, 0)])


def both_halves(mine, axis):
    other = swap(mine, "dp")
    first = lax.axis_index("dp") == 0
    return lax.optimization_barrier(
        jnp.concatenate(
            [jnp.where(first, mine, other), jnp.where(first, other, mine)], axis=axis
        )
    )


def exchange(x, axes):
    return lax.all_to_all(x, axes, split_axis=0, concat_axis=0, tiled=True)


def along_line(x, pairs):
    return lax.ppermute(x, "tensor", pairs)


def line_steps():
    n = lax.axis_size("tensor")
    right = [(i, i + 1) for i in range(n - 1)]
    left = [(i + 1, i) for i in range(n - 1)]
    twice = [(i, (i + 2) % n) for i in range(n)]
    return n, right, left, twice


def line_gather(x):
    n, right, left, twice = line_steps()
    t = lax.axis_index("tensor")
    two = along_line(x, twice)
    from_left, from_right = along_line(x, right), along_line(x, left)
    three = along_line(two, [(n - 2, n - 1), (1, 0)])
    return [x, jnp.where(t == 0, three, from_left), two, jnp.where(t == n - 1, three, from_right)]


def unit_gradients(gate, up, dhid):
    sigma = jax.nn.sigmoid(gate)
    silu_gate = gate * sigma
    act = (silu_gate * up).astype(BF)
    d_up = (dhid * silu_gate).astype(BF)
    d_gate = (dhid * up * sigma * (1.0 + gate * (1.0 - sigma))).astype(BF)
    return act, d_gate, d_up


def reduced_rows(d_gate, d_up, gate_full, up_full, part):
    n = lax.axis_size("tensor")
    t = lax.axis_index("tensor")

    def row_part(index):
        return dot(d_gate, cut(gate_full, index, part, 0), 1, 1) + dot(
            d_up, cut(up_full, index, part, 0), 1, 1
        )

    n, right, left, twice = line_steps()
    edge = row_part(jnp.where(t == 0, n - 1, 0)).astype(BF)
    edge = along_line(edge, [(0, 1), (n - 1, n - 2)])
    from_left = along_line(row_part((t + 1) % n).astype(BF), right)
    from_right = along_line(row_part((t - 1) % n).astype(BF), left)
    own_two = row_part((t + 2) % n)
    own = row_part(t)
    from_two = along_line((own_two + edge.astype(F32)).astype(BF), twice)
    total = own + from_left.astype(F32) + from_right.astype(F32) + from_two.astype(F32)
    return total.astype(BF)


def inner(grad_out, layer_in, routes, combine, gate_weight, up_weight, down_weight):
    cols = lax.axis_size("col")
    n = lax.axis_size("tensor")
    tokens, width = grad_out.shape
    rows = cols * CAP
    half = width // 2
    part = width // n
    per_half = half // part
    my_dp = lax.axis_index("dp")
    my_zh = lax.axis_index("zh")
    t = lax.axis_index("tensor")

    routes_t = routes.T
    far_routes = swap(routes_t, "zh")
    far_tokens = swap(cut(layer_in, t, part, 1), "zh")

    ids = jnp.arange(cols, dtype=jnp.int32)
    near_labels = my_zh * cols + ids
    labels = jnp.concatenate([near_labels, (1 - my_zh) * cols + ids])
    picker, factor = slot_tables(routes_t, combine.T, labels)
    near_picker, far_picker = picker[:rows], picker[rows:]

    def sent(x):
        return x.reshape(cols, CAP, x.shape[1])

    far_grad = pick_scaled(far_picker, cut(grad_out, t, part, 1), factor[rows:])
    far_grad = exchange(sent(far_grad), "col").reshape(rows, part)
    far_grad = swap(far_grad, "zh")

    near_sent = jnp.concatenate(
        [
            sent(pick(near_picker, layer_in)),
            sent(pick_scaled(near_picker, grad_out, factor[:rows])),
        ],
        axis=1,
    )
    far_routes, _ = lax.optimization_barrier((far_routes, far_picker))
    arriving_picker, _ = slot_tables(far_routes, None, near_labels)
    far_in = exchange(sent(pick(arriving_picker, far_tokens)), "col")
    far_in = far_in.reshape(rows, part)
    near_got = exchange(near_sent, "col")
    near_in = near_got[:, :CAP].reshape(rows, width)
    near_grad = near_got[:, CAP:].reshape(rows, width)

    gate_full = both_halves(gate_weight[0], 0)
    up_full = both_halves(up_weight[0], 0)
    down_full = both_halves(down_weight[0], 1)

    far_ins = line_gather(far_in)
    far_grads = line_gather(far_grad)

    act, d_gate, d_up = unit_gradients(
        dot(near_in, gate_full, 1, 0),
        dot(near_in, up_full, 1, 0),
        dot(near_grad, down_full, 1, 1),
    )
    near_rows = reduced_rows(d_gate, d_up, gate_full, up_full, part)

    gate = up = dhid = 0.0
    for s in (0, 2, 1, 3):
        q = (t - s) % n
        gate = gate + dot(far_ins[s], cut(gate_full, q, part, 0), 1, 0)
        up = up + dot(far_ins[s], cut(up_full, q, part, 0), 1, 0)
        dhid = dhid + dot(far_grads[s], cut(down_full, q, part, 1), 1, 1)
    far_act, far_d_gate, far_d_up = unit_gradients(gate, up, dhid)
    far_rows = reduced_rows(far_d_gate, far_d_up, gate_full, up_full, part)

    first = my_zh == 0
    back = jnp.stack(
        [jnp.where(first, near_rows, far_rows), jnp.where(first, far_rows, near_rows)]
    )
    back = exchange(back.reshape(2 * cols, CAP, part), ("zh", "col"))
    back = back.reshape(2, rows, part)
    total = dot(near_picker, cut(back, my_zh, 1, 0)[0], 0, 0) + dot(
        far_picker, cut(back, 1 - my_zh, 1, 0)[0], 0, 0
    )
    total = total.astype(BF)

    far_in_all = jnp.stack(far_ins)
    far_grad_all = jnp.stack(far_grads)

    def quarter(stacked, q):
        return cut(stacked, (t - q) % n, 1, 0)[0]

    def in_term(h, near_d, far_d):
        near = dot(cut(near_in, h, half, 1), near_d, 0, 0)
        far = [dot(quarter(far_in_all, per_half * h + k), far_d, 0, 0) for k in range(per_half)]
        return ((near + jnp.concatenate(far, axis=0)) * 0.25).astype(BF)

    def down_term(h, near_a, far_a):
        near = dot(near_a, cut(near_grad, h, half, 1), 0, 0)
        far = [dot(far_a, quarter(far_grad_all, per_half * h + k), 0, 0) for k in range(per_half)]
        return ((near + jnp.concatenate(far, axis=1)) * 0.25).astype(BF)

    def finish(term, near_side, far_side):
        got_term = swap(term(1 - my_dp, near_side, far_side), "dp")
        return (term(my_dp, near_side, far_side).astype(F32) + got_term.astype(F32)).astype(BF)

    grad_gate = finish(in_term, d_gate, far_d_gate)
    grad_up = finish(in_term, d_up, far_d_up)
    grad_down = finish(down_term, act, far_act)
    total, grad_gate, grad_up, grad_down = lax.optimization_barrier(
        (total, grad_gate, grad_up, grad_down)
    )
    total = lax.all_gather(total, "tensor", axis=0, tiled=False)
    total = jnp.transpose(total, (1, 0, 2)).reshape(tokens, width)
    return total, grad_gate[None], grad_up[None], grad_down[None]


def solution(mesh):
    n_dp, n_expert, n_tensor = (mesh.shape[a] for a in ("dp", "expert", "tensor"))
    split = Mesh(
        mesh.devices.reshape(n_dp, 2, n_expert // 2, n_tensor), ("dp", "zh", "col", "tensor")
    )
    blocks = P(("dp", "zh", "col"), None)
    by_rows = P(("zh", "col"), "dp", "tensor")
    by_columns = P(("zh", "col"), "tensor", "dp")
    return jax.shard_map(
        inner,
        mesh=split,
        in_specs=(blocks, blocks, blocks, blocks, by_rows, by_rows, by_columns),
        out_specs=(blocks, by_rows, by_rows, by_columns),
        check_vma=False,
    )
```

```python
import jax
import jax.numpy as jnp
from jax import lax
from jax.sharding import Mesh
from jax.sharding import PartitionSpec as P


CAP = 8
BF = jnp.bfloat16
F32 = jnp.float32


def dot(a, b, ca, cb):
    return lax.dot_general(a, b, (((ca,), (cb,)), ((), ())), preferred_element_type=F32)


def cut(x, index, size, axis):
    return lax.dynamic_slice_in_dim(x, index * size, size, axis=axis)


def slot_tables(routes_t, combine_t, labels):
    tokens = routes_t.shape[1]
    experts = labels.shape[0]
    hits = routes_t[None, :, :] == labels[:, None, None]
    chosen = jnp.sum(hits.astype(F32), axis=1)
    scale = jnp.sum(jnp.where(hits, combine_t[None, :, :], 0.0), axis=1)
    ids = jnp.arange(tokens, dtype=jnp.int32)
    earlier = (ids[:, None] < ids[None, :]).astype(BF)
    before = jnp.dot(chosen.astype(BF), earlier, preferred_element_type=F32)
    slots = jnp.arange(CAP, dtype=F32)
    taken = (before[:, None, :] == slots[None, :, None]) & (chosen[:, None, :] > 0)
    factor = jnp.sum(jnp.where(taken, scale[:, None, :], 0.0), axis=2)
    return taken.astype(BF).reshape(experts * CAP, tokens), factor.reshape(experts * CAP, 1)


def picked(picker, factor, layer_in, grad_out, cols):
    width = layer_in.shape[1]
    in_rows = jnp.dot(picker, layer_in, preferred_element_type=F32).astype(BF)
    grad_rows = (jnp.dot(picker, grad_out, preferred_element_type=F32) * factor).astype(BF)
    return jnp.concatenate(
        [in_rows.reshape(cols, CAP, width), grad_rows.reshape(cols, CAP, width)], axis=1
    )


def swap(x, axis):
    return lax.ppermute(x, axis, [(0, 1), (1, 0)])


def mirrored(x):
    last = 2 * lax.axis_size("tensor") - 1
    return lax.ppermute(x, ("zh", "tensor"), [(z, last - z) for z in range(last + 1)])


def both_halves(mine, axis):
    other = swap(mine, "dp")
    first = lax.axis_index("dp") == 0
    return lax.optimization_barrier(
        jnp.concatenate(
            [jnp.where(first, mine, other), jnp.where(first, other, mine)], axis=axis
        )
    )


def exchange(x, axes):
    return lax.all_to_all(x, axes, split_axis=0, concat_axis=0, tiled=True)


def rotated(x, step):
    n = lax.axis_size("tensor")
    return lax.ppermute(x, "tensor", [(i, (i + step) % n) for i in range(n)])


def unit_gradients(gate, up, dhid):
    sigma = jax.nn.sigmoid(gate)
    silu_gate = gate * sigma
    act = (silu_gate * up).astype(BF)
    d_up = (dhid * silu_gate).astype(BF)
    d_gate = (dhid * up * sigma * (1.0 + gate * (1.0 - sigma))).astype(BF)
    return act, d_gate, d_up


def reduced_rows(d_gate, d_up, gate_full, up_full, part, owned):
    n = lax.axis_size("tensor")
    t = lax.axis_index("tensor")

    def row_part(rank):
        g, u = cut(gate_full, owned(rank), part, 0), cut(up_full, owned(rank), part, 0)
        return dot(d_gate, g, 1, 1) + dot(d_up, u, 1, 1)

    received = [rotated(row_part((t + s) % n).astype(BF), s) for s in (2, 1, 3)]
    total = row_part(t)
    for piece in received:
        total = total + piece.astype(F32)
    return total.astype(BF)


def inner(grad_out, layer_in, routes, combine, gate_weight, up_weight, down_weight):
    cols = lax.axis_size("col")
    n = lax.axis_size("tensor")
    tokens, width = grad_out.shape
    rows = cols * CAP
    half = width // 2
    part = width // n
    per_half = half // part
    my_dp = lax.axis_index("dp")
    my_zh = lax.axis_index("zh")
    t = lax.axis_index("tensor")

    ids = jnp.arange(cols, dtype=jnp.int32)
    labels = jnp.concatenate([my_zh * cols + ids, (1 - my_zh) * cols + ids])
    picker, factor = slot_tables(routes.T, combine.T, labels)
    near_picker, far_picker = picker[:rows], picker[rows:]

    far_sent = picked(
        far_picker, factor[rows:], cut(layer_in, t, part, 1), cut(grad_out, t, part, 1), cols
    )
    far_got = exchange(far_sent, "col")
    far_in = mirrored(far_got[:, :CAP].reshape(rows, part))
    far_grad = mirrored(far_got[:, CAP:].reshape(rows, part))

    near_got = exchange(picked(near_picker, factor[:rows], layer_in, grad_out, cols), "col")
    near_in = near_got[:, :CAP].reshape(rows, width)
    near_grad = near_got[:, CAP:].reshape(rows, width)

    gate_full = both_halves(gate_weight[0], 0)
    up_full = both_halves(up_weight[0], 0)
    down_full = both_halves(down_weight[0], 1)

    far_ins = [far_in] + [rotated(far_in, s) for s in range(1, n)]
    far_grads = [far_grad] + [rotated(far_grad, s) for s in range(1, n)]

    act, d_gate, d_up = unit_gradients(
        dot(near_in, gate_full, 1, 0),
        dot(near_in, up_full, 1, 0),
        dot(near_grad, down_full, 1, 1),
    )
    near_rows = reduced_rows(d_gate, d_up, gate_full, up_full, part, lambda r: r)

    gate = up = dhid = 0.0
    for s in range(n):
        q = n - 1 - (t - s) % n
        gate = gate + dot(far_ins[s], cut(gate_full, q, part, 0), 1, 0)
        up = up + dot(far_ins[s], cut(up_full, q, part, 0), 1, 0)
        dhid = dhid + dot(far_grads[s], cut(down_full, q, part, 1), 1, 1)
    far_act, far_d_gate, far_d_up = unit_gradients(gate, up, dhid)
    far_rows = reduced_rows(
        far_d_gate, far_d_up, gate_full, up_full, part, lambda r: n - 1 - r
    )

    def returned(x):
        return exchange(x.reshape(cols, CAP, part), "col").reshape(rows, part)

    far_back = returned(far_rows)
    far_back = mirrored(far_back)
    near_back = returned(near_rows)
    total = (dot(near_picker, near_back, 0, 0) + dot(far_picker, far_back, 0, 0)).astype(BF)

    far_in_all, far_grad_all = jnp.stack(far_ins), jnp.stack(far_grads)

    def quarter(stacked, q):
        return cut(stacked, (t + q + 1) % n, 1, 0)[0]

    def in_term(h, near_d, far_d):
        near = dot(cut(near_in, h, half, 1), near_d, 0, 0)
        far = [dot(quarter(far_in_all, per_half * h + k), far_d, 0, 0) for k in range(per_half)]
        return ((near + jnp.concatenate(far, axis=0)) * 0.25).astype(BF)

    def down_term(h, near_a, far_a):
        near = dot(near_a, cut(near_grad, h, half, 1), 0, 0)
        far = [dot(far_a, quarter(far_grad_all, per_half * h + k), 0, 0) for k in range(per_half)]
        return ((near + jnp.concatenate(far, axis=1)) * 0.25).astype(BF)

    def finish(term, near_side, far_side):
        got_term = swap(term(1 - my_dp, near_side, far_side), "dp")
        return (term(my_dp, near_side, far_side).astype(F32) + got_term.astype(F32)).astype(BF)

    grad_gate = finish(in_term, d_gate, far_d_gate)
    grad_up = finish(in_term, d_up, far_d_up)
    grad_down = finish(down_term, act, far_act)
    total, grad_gate, grad_up, grad_down = lax.optimization_barrier(
        (total, grad_gate, grad_up, grad_down)
    )
    total = lax.all_gather(total, "tensor", axis=0, tiled=False)
    total = jnp.transpose(total, (1, 0, 2)).reshape(tokens, width)
    return total, grad_gate[None], grad_up[None], grad_down[None]


def solution(mesh):
    n_dp, n_expert, n_tensor = (mesh.shape[a] for a in ("dp", "expert", "tensor"))
    split = Mesh(
        mesh.devices.reshape(n_dp, 2, n_expert // 2, n_tensor), ("dp", "zh", "col", "tensor")
    )
    blocks = P(("dp", "zh", "col"), None)
    by_rows = P(("zh", "col"), "dp", "tensor")
    by_columns = P(("zh", "col"), "tensor", "dp")
    return jax.shard_map(
        inner,
        mesh=split,
        in_specs=(blocks, blocks, blocks, blocks, by_rows, by_rows, by_columns),
        out_specs=(blocks, by_rows, by_rows, by_columns),
        check_vma=False,
    )
```

```python
import jax
import jax.numpy as jnp
from jax import lax
from jax.sharding import Mesh
from jax.sharding import PartitionSpec as P


CAP = 8
BF = jnp.bfloat16
F32 = jnp.float32


def dot(a, b, ca, cb):
    return lax.dot_general(a, b, (((ca,), (cb,)), ((), ())), preferred_element_type=F32)


def cut(x, index, size, axis):
    return lax.dynamic_slice_in_dim(x, index * size, size, axis=axis)


def slot_tables(routes_t, combine_t, labels):
    tokens = routes_t.shape[1]
    experts = labels.shape[0]
    hits = routes_t[None, :, :] == labels[:, None, None]
    chosen = jnp.sum(hits.astype(F32), axis=1)
    scale = jnp.sum(jnp.where(hits, combine_t[None, :, :], 0.0), axis=1)
    ids = jnp.arange(tokens, dtype=jnp.int32)
    earlier = (ids[:, None] < ids[None, :]).astype(BF)
    before = jnp.dot(chosen.astype(BF), earlier, preferred_element_type=F32)
    slots = jnp.arange(CAP, dtype=F32)
    taken = (before[:, None, :] == slots[None, :, None]) & (chosen[:, None, :] > 0)
    factor = jnp.sum(jnp.where(taken, scale[:, None, :], 0.0), axis=2)
    return taken.astype(BF).reshape(experts * CAP, tokens), factor.reshape(experts * CAP, 1)


def picked(picker, factor, layer_in, grad_out, cols):
    width = layer_in.shape[1]
    in_rows = jnp.dot(picker, layer_in, preferred_element_type=F32).astype(BF)
    grad_rows = (jnp.dot(picker, grad_out, preferred_element_type=F32) * factor).astype(BF)
    return jnp.concatenate(
        [in_rows.reshape(cols, CAP, width), grad_rows.reshape(cols, CAP, width)], axis=1
    )


def swap(x, axis):
    return lax.ppermute(x, axis, [(0, 1), (1, 0)])


def mirrored(x):
    last = 2 * lax.axis_size("tensor") - 1
    return lax.ppermute(x, ("zh", "tensor"), [(z, last - z) for z in range(last + 1)])


def both_halves(mine, axis):
    other = swap(mine, "dp")
    first = lax.axis_index("dp") == 0
    return lax.optimization_barrier(
        jnp.concatenate(
            [jnp.where(first, mine, other), jnp.where(first, other, mine)], axis=axis
        )
    )


def exchange(x, axes):
    return lax.all_to_all(x, axes, split_axis=0, concat_axis=0, tiled=True)


def rotated(x, step):
    n = lax.axis_size("tensor")
    return lax.ppermute(x, "tensor", [(i, (i + step) % n) for i in range(n)])


def unit_gradients(gate, up, dhid):
    sigma = jax.nn.sigmoid(gate)
    silu_gate = gate * sigma
    act = (silu_gate * up).astype(BF)
    d_up = (dhid * silu_gate).astype(BF)
    d_gate = (dhid * up * sigma * (1.0 + gate * (1.0 - sigma))).astype(BF)
    return act, d_gate, d_up


def reduced_rows(d_gate, d_up, gate_full, up_full, part, owned):
    n = lax.axis_size("tensor")
    t = lax.axis_index("tensor")

    def row_part(rank):
        g, u = cut(gate_full, owned(rank), part, 0), cut(up_full, owned(rank), part, 0)
        return dot(d_gate, g, 1, 1) + dot(d_up, u, 1, 1)

    received = [rotated(row_part((t + s) % n).astype(BF), s) for s in (2, 1, 3)]
    total = row_part(t)
    for piece in received:
        total = total + piece.astype(F32)
    return total.astype(BF)


def inner(grad_out, layer_in, routes, combine, gate_weight, up_weight, down_weight):
    cols = lax.axis_size("col")
    n = lax.axis_size("tensor")
    tokens, width = grad_out.shape
    rows = cols * CAP
    half = width // 2
    part = width // n
    per_half = half // part
    my_dp = lax.axis_index("dp")
    my_zh = lax.axis_index("zh")
    t = lax.axis_index("tensor")

    ids = jnp.arange(cols, dtype=jnp.int32)
    labels = jnp.concatenate([my_zh * cols + ids, (1 - my_zh) * cols + ids])
    picker, factor = slot_tables(routes.T, combine.T, labels)
    near_picker, far_picker = picker[:rows], picker[rows:]

    far_sent = picked(
        far_picker, factor[rows:], cut(layer_in, t, part, 1), cut(grad_out, t, part, 1), cols
    )
    far_got = exchange(far_sent, "col")
    far_in = mirrored(far_got[:, :CAP].reshape(rows, part))
    far_grad = mirrored(far_got[:, CAP:].reshape(rows, part))

    near_got = exchange(picked(near_picker, factor[:rows], layer_in, grad_out, cols), "col")
    near_in = near_got[:, :CAP].reshape(rows, width)
    near_grad = near_got[:, CAP:].reshape(rows, width)

    gate_full = both_halves(gate_weight[0], 0)
    up_full = both_halves(up_weight[0], 0)
    down_full = both_halves(down_weight[0], 1)

    far_ins = [far_in] + [rotated(far_in, s) for s in range(1, n)]
    far_grads = [far_grad] + [rotated(far_grad, s) for s in range(1, n)]

    act, d_gate, d_up = unit_gradients(
        dot(near_in, gate_full, 1, 0),
        dot(near_in, up_full, 1, 0),
        dot(near_grad, down_full, 1, 1),
    )
    near_rows = (dot(d_gate, gate_full, 1, 1) + dot(d_up, up_full, 1, 1)).astype(BF)
    near_back = exchange(near_rows.reshape(cols, CAP, width), "col").reshape(rows, width)
    near_sum = dot(near_picker, near_back, 0, 0).astype(BF)
    near_parts = [rotated(cut(near_sum, (t + s) % n, part, 1), s) for s in (2, 1, 3)]

    gate = up = dhid = 0.0
    for s in range(n):
        q = n - 1 - (t - s) % n
        gate = gate + dot(far_ins[s], cut(gate_full, q, part, 0), 1, 0)
        up = up + dot(far_ins[s], cut(up_full, q, part, 0), 1, 0)
        dhid = dhid + dot(far_grads[s], cut(down_full, q, part, 1), 1, 1)
    far_act, far_d_gate, far_d_up = unit_gradients(gate, up, dhid)
    far_rows = reduced_rows(
        far_d_gate, far_d_up, gate_full, up_full, part, lambda r: n - 1 - r
    )

    def returned(x):
        return exchange(x.reshape(cols, CAP, part), "col").reshape(rows, part)

    far_back = returned(far_rows)
    far_back = mirrored(far_back)
    total = cut(near_sum, t, part, 1).astype(F32)
    for piece in near_parts:
        total = total + piece.astype(F32)
    total = (total + dot(far_picker, far_back, 0, 0)).astype(BF)

    far_in_all = jnp.stack(far_ins)
    far_grad_all = jnp.stack(far_grads)

    def quarter(stacked, q):
        return cut(stacked, (t + q + 1) % n, 1, 0)[0]

    def in_term(h, near_d, far_d):
        near = dot(cut(near_in, h, half, 1), near_d, 0, 0)
        far = [dot(quarter(far_in_all, per_half * h + k), far_d, 0, 0) for k in range(per_half)]
        return ((near + jnp.concatenate(far, axis=0)) * 0.25).astype(BF)

    def down_term(h, near_a, far_a):
        near = dot(near_a, cut(near_grad, h, half, 1), 0, 0)
        far = [dot(far_a, quarter(far_grad_all, per_half * h + k), 0, 0) for k in range(per_half)]
        return ((near + jnp.concatenate(far, axis=1)) * 0.25).astype(BF)

    def finish(term, near_side, far_side):
        got_term = swap(term(1 - my_dp, near_side, far_side), "dp")
        return (term(my_dp, near_side, far_side).astype(F32) + got_term.astype(F32)).astype(BF)

    grad_gate = finish(in_term, d_gate, far_d_gate)
    grad_up = finish(in_term, d_up, far_d_up)
    grad_down = finish(down_term, act, far_act)
    total, grad_gate, grad_up, grad_down = lax.optimization_barrier(
        (total, grad_gate, grad_up, grad_down)
    )
    total = lax.all_gather(total, "tensor", axis=0, tiled=False)
    total = jnp.transpose(total, (1, 0, 2)).reshape(tokens, width)
    return total, grad_gate[None], grad_up[None], grad_down[None]


def solution(mesh):
    n_dp, n_expert, n_tensor = (mesh.shape[a] for a in ("dp", "expert", "tensor"))
    split = Mesh(
        mesh.devices.reshape(n_dp, 2, n_expert // 2, n_tensor), ("dp", "zh", "col", "tensor")
    )
    blocks = P(("dp", "zh", "col"), None)
    by_rows = P(("zh", "col"), "dp", "tensor")
    by_columns = P(("zh", "col"), "tensor", "dp")
    return jax.shard_map(
        inner,
        mesh=split,
        in_specs=(blocks, blocks, blocks, blocks, by_rows, by_rows, by_columns),
        out_specs=(blocks, by_rows, by_rows, by_columns),
        check_vma=False,
    )
```
